128 devices in a mesh: farcp: 4 (over x_lo, core), nearcp: 4 (over z_lo, x_hi), heads: 8 (over z_hi, y).
Axes of the slice: x: 4 (x_hi: 2, x_lo: 2; x = x_hi * 2 + x_lo), y: 4, z: 4 (z_hi: 2, z_lo: 2; z = z_hi * 2 + z_lo), core: 2. Of those that a mesh axis runs over, the one named last changes fastest.
Arguments:
- raw_keys: bfloat16 [16, 24576, 8, 128], P(None, ('farcp', 'nearcp'), 'heads'), may hold values from -6 to 6
- raw_values: bfloat16 [16, 24576, 8, 128], P(None, ('farcp', 'nearcp'), 'heads'), may hold values from -6 to 6
- turn_angle: float32 [24576, 64], replicated, may hold values from -3.140625 to 3.140625
Outputs:
- stored_keys: bfloat16 [16, 8, 128, 24576], P(('farcp', 'nearcp'), 'heads')
- stored_values: bfloat16 [16, 24576, 8, 128], P(('farcp', 'nearcp'), None, 'heads')
- page_high: bfloat16 [16, 384, 8, 128], P(('farcp', 'nearcp'), None, 'heads')
- page_low: bfloat16 [16, 384, 8, 128], P(('farcp', 'nearcp'), None, 'heads')
The draws below stay inside these ranges and needn't reach their ends.
All inputs are finite; a program needn't handle non-finite values.
Results may differ from the reference program's by a relative error of at most 0.001.
Values may be sent and summed in bfloat16 or wider, within the bound.
A program may use at most 128 MiB of HBM per device.

```python
import jax
import jax.numpy as jnp

BATCH = 16
LENGTH = 24576
KV_HEADS = 8
HEAD_SIZE = 128
HALF_HEAD = 64
PAGE = 64


def shard_levels(own_key, dims, cuts, smallest, high):
    def one(dim, blocks):
        steps = jax.random.uniform(jax.random.fold_in(jax.random.fold_in(own_key, 6), dim), (blocks,), jnp.float32, smallest / len(cuts), high / len(cuts))
        return jnp.repeat(jnp.exp(steps), dims[dim] // blocks).reshape((-1,) + (1,) * (len(dims) - dim - 1))

    gain = one(*cuts[0])
    for cut in cuts[1:]:
        gain = gain * one(*cut)
    return gain


def bell_draw(rng, extent, width, reach, pieces=(), kind=jnp.bfloat16):
    gain = shard_levels(rng, extent, pieces, -0.22, 0.18) if pieces else 1.0
    array = jax.random.normal(rng, extent, jnp.float32) * width * gain
    return jnp.minimum(jnp.maximum(array, -reach), reach).astype(kind)


def setup_inputs(seed: int = 0) -> dict:
    key_of = jax.random.split(jax.random.key(seed), 4)
    return {
        "raw_keys": bell_draw(key_of[0], (BATCH, LENGTH, KV_HEADS, HEAD_SIZE), 1.0, 6.0, ((1, 16), (2, 8))),
        "raw_values": bell_draw(key_of[1], (BATCH, LENGTH, KV_HEADS, HEAD_SIZE), 1.0, 6.0, ((1, 16), (2, 8))),
        "turn_angle": jnp.clip(jax.random.uniform(key_of[2], (LENGTH, HALF_HEAD), jnp.float32, -3.140625, 3.140625), -3.140625, 3.140625),
    }


def apply_rotary(vectors, angle):
    half = vectors.shape[-1] // 2
    cosine, sine = jnp.cos(angle)[None, :, None, :], jnp.sin(angle)[None, :, None, :]
    first, second = vectors[..., :half], vectors[..., half:]
    return jnp.concatenate([first * cosine - second * sine, second * cosine + first * sine], axis=-1)


def keys_in_place(plain_keys, angle):
    wide_keys = plain_keys.astype(jnp.float32)
    return apply_rotary(wide_keys, angle)


def reference(raw_keys, raw_values, turn_angle):
    turned_keys = keys_in_place(raw_keys, turn_angle)
    narrow_keys = turned_keys.astype(jnp.bfloat16)
    page_view = narrow_keys.reshape(BATCH, LENGTH // PAGE, PAGE, KV_HEADS, HEAD_SIZE)
    page_high = jnp.max(page_view, axis=2)
    page_low = jnp.min(page_view, axis=2)
    stored_keys = jnp.transpose(narrow_keys, (0, 2, 3, 1))
    stored_values = raw_values
    return stored_keys, stored_values, page_high, page_low
```

```python
import functools

import jax
import jax.numpy as jnp
from jax import lax
from jax.experimental import pallas as pl
from jax.experimental.pallas import tpu as pltpu
from jax.sharding import PartitionSpec as P

PAGE = 64
MESH = pl.DeviceIdType.MESH
ORDER = (
    (2, 1, 0), (2, 0, 0), (2, 1, 1), (2, 0, 1),
    (1, 1, 0), (3, 1, 0), (1, 0, 0), (3, 0, 0),
    (1, 1, 1), (3, 1, 1), (1, 0, 1), (3, 0, 1),
    (0, 1, 0), (0, 1, 1), (0, 0, 1),
)
PIECES = 4
EARLY = 2


def position():
    far, near = lax.axis_index("farcp"), lax.axis_index("nearcp")
    return (near % 2) * 2 + far // 2, near // 2, far % 2


def indices(x, z, core):
    return (x % 2) * 2 + core, z * 2 + x // 2


def exchange(
    keys, values, angle, out_keys, out_values, out_high, out_low,
    block, landed, turn, cosine, sine, high, low,
    send_keys, recv_keys, send_values, recv_values, local,
):
    blocks, rows, size = block.shape
    half = size // 2
    step = rows // PIECES
    x, z, core = position()
    far, near = indices(x, z, core)
    me = far * 4 + near

    def partner(offset):
        dx, dz, dc = offset
        return indices((x + dx) % 4, (z + dz) % 2, (core + dc) % 2)

    barrier = pltpu.get_barrier_semaphore()
    for offset in ORDER:
        f, n = partner(offset)
        pl.semaphore_signal(barrier, inc=1, device_id={"farcp": f, "nearcp": n}, device_id_type=MESH)

    first = pl.multiple_of(me * rows, 128)
    get_angle = pltpu.make_async_copy(angle.at[:, pl.ds(first, rows)], turn, local.at[0])
    get_angle.start()
    get_keys = pltpu.make_async_copy(keys, block, local.at[1])
    get_keys.start()
    own_values = pltpu.make_async_copy(values.at[me], out_values.at[me], local.at[2])
    own_values.start()
    pl.semaphore_wait(barrier, len(ORDER))

    def copy(source, target, send, recv, which, piece):
        f, n = partner(ORDER[which])
        part = pl.ds(piece * step, step)
        return pltpu.make_async_remote_copy(
            source.at[f * 4 + n, part],
            target.at[me, part],
            send.at[which * PIECES + piece],
            recv.at[which * PIECES + piece],
            device_id={"farcp": f, "nearcp": n},
            device_id_type=MESH,
        )

    value_copies, key_copies = [], []
    for piece in range(EARLY):
        for which in range(len(ORDER)):
            value_copies.append(copy(values, out_values, send_values, recv_values, which, piece))
            value_copies[-1].start()

    get_angle.wait()
    c, s = jnp.cos(turn[...]), jnp.sin(turn[...])
    cosine[...] = jnp.concatenate([c, c], axis=0).T
    sine[...] = jnp.concatenate([-s, s], axis=0).T
    get_keys.wait()

    tile = 128
    tiles = rows // tile

    @pl.loop(0, tiles)
    def _(t):
        at = pl.ds(pl.multiple_of(t * tile, tile), tile)
        co, si = cosine[at], sine[at]

        @pl.loop(0, blocks)
        def _(b):
            k = block[b, at].astype(jnp.float32)
            block[b, at] = (k * co + pltpu.roll(k, half, 1) * si).astype(block.dtype)

    @pl.loop(0, tiles)
    def _(t):
        at = pl.ds(pl.multiple_of(t * tile, tile), tile)
        landed[me, at] = block[me, at]

    for piece in range(PIECES):
        for which in range(len(ORDER)):
            key_copies.append(copy(block, landed, send_keys, recv_keys, which, piece))
            key_copies[-1].start()
    for piece in range(EARLY, PIECES):
        for which in range(len(ORDER)):
            value_copies.append(copy(values, out_values, send_values, recv_values, which, piece))
            value_copies[-1].start()

    for one in key_copies:
        one.wait_recv()

    chunk = 8 * PAGE

    @pl.loop(0, blocks * (rows // chunk))
    def _(i):
        b, t = i // (rows // chunk), i % (rows // chunk)
        k = landed[b, pl.ds(pl.multiple_of(t * chunk, chunk), chunk)]
        for j in range(chunk // tile):
            out_keys[:, pl.ds(pl.multiple_of(i * chunk + j * tile, tile), tile)] = k[j * tile : (j + 1) * tile].T
        pages = k.astype(jnp.float32).reshape(chunk // PAGE, PAGE, size)
        to = pl.ds(pl.multiple_of(i * 8, 8), 8)
        high[to] = jnp.max(pages, axis=1)
        low[to] = jnp.min(pages, axis=1)

    out_high[...] = high[...].astype(out_high.dtype)
    out_low[...] = low[...].astype(out_low.dtype)

    own_values.wait()
    for one in value_copies:
        one.wait_recv()
    for one in key_copies + value_copies:
        one.wait_send()


def per_device(raw_keys, raw_values, turn_angle):
    blocks, rows, _, size = raw_keys.shape
    length = blocks * rows
    kind = raw_keys.dtype
    keys = raw_keys.reshape(blocks, rows, size)
    values = raw_values.reshape(blocks, rows, size)
    angle = turn_angle.T
    anywhere = pl.BlockSpec(memory_space=pl.ANY)
    inside = pl.BlockSpec(memory_space=pltpu.VMEM)
    many = len(ORDER) * PIECES
    moved = pl.pallas_call(
        exchange,
        out_shape=(
            pltpu.VMEM((size, length), kind),
            pltpu.VMEM((blocks, rows, size), kind),
            pltpu.VMEM((length // PAGE, size), kind),
            pltpu.VMEM((length // PAGE, size), kind),
        ),
        in_specs=[anywhere] * 3,
        out_specs=(inside,) * 4,
        scratch_shapes=[
            pltpu.VMEM((blocks, rows, size), kind),
            pltpu.VMEM((blocks, rows, size), kind),
            pltpu.VMEM((size // 2, rows), jnp.float32),
            pltpu.VMEM((rows, size), jnp.float32),
            pltpu.VMEM((rows, size), jnp.float32),
            pltpu.VMEM((length // PAGE, size), jnp.float32),
            pltpu.VMEM((length // PAGE, size), jnp.float32),
        ]
        + [pltpu.SemaphoreType.DMA((many,))] * 4
        + [pltpu.SemaphoreType.DMA((3,))],
        compiler_params=pltpu.CompilerParams(
            collective_id=0, has_side_effects=True, vmem_limit_bytes=48 << 20
        ),
    )(keys, values, angle)
    k, v, high, low = moved
    return k[None, None], v.reshape(1, length, 1, size), high[None, :, None], low[None, :, None]


def solution(mesh):
    return jax.shard_map(
        per_device,
        mesh=mesh,
        in_specs=(
            P(None, ("farcp", "nearcp"), "heads", None),
            P(None, ("farcp", "nearcp"), "heads", None),
            P(),
        ),
        out_specs=(
            P(("farcp", "nearcp"), "heads", None, None),
            P(("farcp", "nearcp"), None, "heads", None),
            P(("farcp", "nearcp"), None, "heads", None),
            P(("farcp", "nearcp"), None, "heads", None),
        ),
        check_vma=False,
    )
```

```python
import functools

import jax
import jax.numpy as jnp
from jax import lax
from jax.experimental import pallas as pl
from jax.experimental.pallas import tpu as pltpu
from jax.sharding import PartitionSpec as P

PAGE = 64
MESH = pl.DeviceIdType.MESH
ORDER = (
    (2, 1, 0, 0), (2, 0, 0, 0), (2, 1, 1, 0), (2, 0, 1, 0),
    (1, 1, 0, 0), (3, 1, 0, 0), (1, 0, 0, 0), (3, 0, 0, 0),
    (1, 1, 1, 0), (3, 1, 1, 0), (1, 0, 1, 0), (3, 0, 1, 0),
    (0, 1, 0, 0), (0, 1, 1, 0), (0, 0, 1, 0),
)
PIECES = 4
EARLY = 2


def position():
    far, near = lax.axis_index("farcp"), lax.axis_index("nearcp")
    return (near % 2) * 2 + far // 2, near // 2, far % 2


def indices(x, z, core):
    return (x % 2) * 2 + core, z * 2 + x // 2


def exchange(
    keys, values, angle, out_keys, out_values, out_high, out_low,
    staged, block, landed, turn, cosine, sine, high, low,
    send_keys, recv_keys, send_values, recv_values, local,
):
    blocks, rows, size = block.shape
    half = size // 2
    step = rows // PIECES
    x, z, core = position()
    far, near = indices(x, z, core)
    me = far * 4 + near

    def partner(offset):
        dx, dz, dc, turned = offset
        return indices((x + dx) % 4, (z + dz + turned * core) % 2, (core + dc) % 2)

    get_values = pltpu.make_async_copy(values.at[:, pl.ds(0, EARLY * step)], staged, local.at[3])
    get_values.start()
    barrier = pltpu.get_barrier_semaphore()
    for offset in ORDER:
        f, n = partner(offset)
        pl.semaphore_signal(barrier, inc=1, device_id={"farcp": f, "nearcp": n}, device_id_type=MESH)

    first = pl.multiple_of(me * rows, 128)
    get_angle = pltpu.make_async_copy(angle.at[:, pl.ds(first, rows)], turn, local.at[0])
    get_angle.start()
    get_keys = pltpu.make_async_copy(keys, block, local.at[1])
    get_keys.start()
    own_values = pltpu.make_async_copy(values.at[me], out_values.at[me], local.at[2])
    own_values.start()
    pl.semaphore_wait(barrier, len(ORDER))
    get_values.wait()

    def copy(source, target, send, recv, which, piece):
        f, n = partner(ORDER[which])
        part = pl.ds(piece * step, step)
        return pltpu.make_async_remote_copy(
            source.at[f * 4 + n, part],
            target.at[me, part],
            send,
            recv,
            device_id={"farcp": f, "nearcp": n},
            device_id_type=MESH,
        )

    for piece in range(EARLY):
        for which in range(len(ORDER)):
            copy(staged, out_values, send_values, recv_values, which, piece).start()

    get_angle.wait()
    c, s = jnp.cos(turn[...]), jnp.sin(turn[...])
    cosine[...] = jnp.concatenate([c, c], axis=0).T
    sine[...] = jnp.concatenate([-s, s], axis=0).T
    get_keys.wait()

    tile = 128
    tiles = rows // tile

    @pl.loop(0, tiles)
    def _(t):
        at = pl.ds(pl.multiple_of(t * tile, tile), tile)
        co, si = cosine[at], sine[at]

        @pl.loop(0, blocks)
        def _(b):
            k = block[b, at].astype(jnp.float32)
            block[b, at] = (k * co + pltpu.roll(k, half, 1) * si).astype(block.dtype)

    @pl.loop(0, tiles)
    def _(t):
        at = pl.ds(pl.multiple_of(t * tile, tile), tile)
        landed[me, at] = block[me, at]

    for piece in range(PIECES):
        for which in range(len(ORDER)):
            copy(block, landed, send_keys, recv_keys, which, piece).start()
    for piece in range(EARLY, PIECES):
        for which in range(len(ORDER)):
            copy(values, out_values, send_values, recv_values, which, piece).start()

    def all_of(source, target, send, recv):
        every = pl.ds(0, len(ORDER))
        return pltpu.make_async_remote_copy(
            source.at[every],
            target.at[every],
            send,
            recv,
            device_id={"farcp": far, "nearcp": near},
            device_id_type=MESH,
        )

    all_keys = all_of(block, landed, send_keys, recv_keys)
    all_values = all_of(values, out_values, send_values, recv_values)
    all_keys.wait_recv()

    chunk = 8 * PAGE

    @pl.loop(0, blocks * (rows // chunk))
    def _(i):
        b, t = i // (rows // chunk), i % (rows // chunk)
        k = landed[b, pl.ds(pl.multiple_of(t * chunk, chunk), chunk)]
        for j in range(chunk // tile):
            out_keys[:, pl.ds(pl.multiple_of(i * chunk + j * tile, tile), tile)] = k[j * tile : (j + 1) * tile].T
        pages = k.astype(jnp.float32).reshape(chunk // PAGE, PAGE, size)
        to = pl.ds(pl.multiple_of(i * 8, 8), 8)
        high[to] = jnp.max(pages, axis=1)
        low[to] = jnp.min(pages, axis=1)

    out_high[...] = high[...].astype(out_high.dtype)
    out_low[...] = low[...].astype(out_low.dtype)

    own_values.wait()
    all_keys.wait_send()
    all_values.wait_send()
    all_values.wait_recv()


def write_out(keys, values, high, low, out_keys, out_values, out_high, out_low, done):
    copies = [(high, out_high), (low, out_low)]
    for a, b in ((keys, out_keys), (values, out_values)):
        step = a.shape[0] // 8
        copies += [(a.at[pl.ds(i * step, step)], b.at[pl.ds(i * step, step)]) for i in range(8)]
    copies = [pltpu.make_async_copy(a, b, done.at[i]) for i, (a, b) in enumerate(copies)]
    for one in copies:
        one.start()
    for one in copies:
        one.wait()


def per_device(raw_keys, raw_values, turn_angle):
    blocks, rows, _, size = raw_keys.shape
    length = blocks * rows
    kind = raw_keys.dtype
    keys = raw_keys.reshape(blocks, rows, size)
    values = raw_values.reshape(blocks, rows, size)
    angle = turn_angle.T
    anywhere = pl.BlockSpec(memory_space=pl.ANY)
    inside = pl.BlockSpec(memory_space=pltpu.VMEM)
    moved = pl.pallas_call(
        exchange,
        out_shape=(
            pltpu.VMEM((size, length), kind),
            pltpu.VMEM((blocks, rows, size), kind),
            pltpu.VMEM((length // PAGE, size), kind),
            pltpu.VMEM((length // PAGE, size), kind),
        ),
        in_specs=[anywhere] * 3,
        out_specs=(inside,) * 4,
        scratch_shapes=[
            pltpu.VMEM((blocks, rows // PIECES * EARLY, size), kind),
            pltpu.VMEM((blocks, rows, size), kind),
            pltpu.VMEM((blocks, rows, size), kind),
            pltpu.VMEM((size // 2, rows), jnp.float32),
            pltpu.VMEM((rows, size), jnp.float32),
            pltpu.VMEM((rows, size), jnp.float32),
            pltpu.VMEM((length // PAGE, size), jnp.float32),
            pltpu.VMEM((length // PAGE, size), jnp.float32),
        ]
        + [pltpu.SemaphoreType.DMA] * 4
        + [pltpu.SemaphoreType.DMA((4,))],
        compiler_params=pltpu.CompilerParams(
            collective_id=0, has_side_effects=True, vmem_limit_bytes=48 << 20
        ),
    )(keys, values, angle)
    k, v, high, low = moved
    moved = [pltpu.with_memory_space_constraint(a, pltpu.VMEM) for a in (k, v.reshape(length, size), high, low)]
    k, v, high, low = pl.pallas_call(
        write_out,
        out_shape=tuple(pltpu.HBM(a.shape, a.dtype) for a in moved),
        in_specs=[inside] * 4,
        out_specs=(anywhere,) * 4,
        scratch_shapes=[pltpu.SemaphoreType.DMA((18,))],
        compiler_params=pltpu.CompilerParams(vmem_limit_bytes=1 << 20),
    )(*moved)
    return k[None, None], v[None, :, None], high[None, :, None], low[None, :, None]


def solution(mesh):
    return jax.shard_map(
        per_device,
        mesh=mesh,
        in_specs=(
            P(None, ("farcp", "nearcp"), "heads", None),
            P(None, ("farcp", "nearcp"), "heads", None),
            P(),
        ),
        out_specs=(
            P(("farcp", "nearcp"), "heads", None, None),
            P(("farcp", "nearcp"), None, "heads", None),
            P(("farcp", "nearcp"), None, "heads", None),
            P(("farcp", "nearcp"), None, "heads", None),
        ),
        check_vma=False,
    )
```

```python
import functools

import jax
import jax.numpy as jnp
from jax import lax
from jax.experimental import pallas as pl
from jax.experimental.pallas import tpu as pltpu
from jax.sharding import PartitionSpec as P

PAGE = 64
MESH = pl.DeviceIdType.MESH
ORDER = (
    (2, 1, 0, 0), (2, 0, 0, 0), (2, 1, 1, 0), (2, 0, 1, 0),
    (1, 1, 0, 0), (3, 1, 0, 0), (1, 0, 0, 0), (3, 0, 0, 0),
    (1, 1, 1, 0), (3, 1, 1, 0), (1, 0, 1, 0), (3, 0, 1, 0),
    (0, 1, 0, 0), (0, 1, 1, 0), (0, 0, 1, 0),
)
PIECES = 8
EARLY = 3


def position():
    far, near = lax.axis_index("farcp"), lax.axis_index("nearcp")
    return (near % 2) * 2 + far // 2, near // 2, far % 2


def indices(x, z, core):
    return (x % 2) * 2 + core, z * 2 + x // 2


def exchange(
    keys, values, angle, out_keys, out_values, out_high, out_low,
    staged, block, landed, turn, cosine, sine, high, low,
    for_early, for_keys, for_across, for_along, local,
):
    blocks, rows, size = block.shape
    half = size // 2
    step = rows // PIECES
    x, z, core = position()
    far, near = indices(x, z, core)
    me = far * 4 + near

    def partner(offset):
        dx, dz, dc, turned = offset
        return indices((x + dx) % 4, (z + dz + turned * core) % 2, (core + dc) % 2)

    get_values = pltpu.make_async_copy(values.at[:, pl.ds(0, EARLY * step)], staged, local.at[3])
    get_values.start()
    barrier = pltpu.get_barrier_semaphore()
    for offset in ORDER:
        f, n = partner(offset)
        pl.semaphore_signal(barrier, inc=1, device_id={"farcp": f, "nearcp": n}, device_id_type=MESH)

    first = pl.multiple_of(me * rows, 128)
    get_angle = pltpu.make_async_copy(angle.at[:, pl.ds(first, rows)], turn, local.at[0])
    get_angle.start()
    get_keys = pltpu.make_async_copy(keys, block, local.at[1])
    get_keys.start()
    own_values = pltpu.make_async_copy(values.at[me], out_values.at[me], local.at[2])
    own_values.start()
    pl.semaphore_wait(barrier, len(ORDER))
    get_values.wait()

    def copy(source, target, semaphores, offset, piece):
        f, n = partner(offset)
        part = pl.ds(piece * step, step)
        return pltpu.make_async_remote_copy(
            source.at[f * 4 + n, part],
            target.at[me, part],
            semaphores.at[0],
            semaphores.at[1],
            device_id={"farcp": f, "nearcp": n},
            device_id_type=MESH,
        )

    for piece in range(EARLY):
        for offset in ORDER:
            copy(staged, out_values, for_early, offset, piece).start()

    get_angle.wait()
    c, s = jnp.cos(turn[...]), jnp.sin(turn[...])
    cosine[...] = jnp.concatenate([c, c], axis=0).T
    sine[...] = jnp.concatenate([-s, s], axis=0).T
    get_keys.wait()

    tile = 128
    tiles = rows // tile

    @pl.loop(0, tiles)
    def _(t):
        at = pl.ds(pl.multiple_of(t * tile, tile), tile)
        co, si = cosine[at], sine[at]

        @pl.loop(0, blocks)
        def _(b):
            k = block[b, at].astype(jnp.float32)
            block[b, at] = (k * co + pltpu.roll(k, half, 1) * si).astype(block.dtype)

    @pl.loop(0, tiles)
    def _(t):
        at = pl.ds(pl.multiple_of(t * tile, tile), tile)
        landed[me, at] = block[me, at]

    for piece in range(PIECES):
        for offset in ORDER:
            copy(block, landed, for_keys, offset, piece).start()
    across = [offset for offset in ORDER if offset[2]]
    along = [offset for offset in ORDER if not offset[2]]
    for piece in range(EARLY, PIECES):
        for offset in across:
            copy(values, out_values, for_across, offset, piece).start()

    @pl.when(core == 1)
    def _():
        for piece in range(EARLY, PIECES):
            for offset in along:
                copy(values, out_values, for_along, offset, piece).start()

    def all_of(source, target, semaphores, partners, pieces):
        every = (pl.ds(0, len(partners)), pl.ds(0, pieces * step))
        return pltpu.make_async_remote_copy(
            source.at[every],
            target.at[every],
            semaphores.at[0],
            semaphores.at[1],
            device_id={"farcp": far, "nearcp": near},
            device_id_type=MESH,
        )

    all_keys = all_of(block, landed, for_keys, ORDER, PIECES)
    all_keys.wait_recv()
    chunk = 8 * PAGE

    @pl.loop(0, blocks * (rows // chunk))
    def _(i):
        b, t = i // (rows // chunk), i % (rows // chunk)
        k = landed[b, pl.ds(pl.multiple_of(t * chunk, chunk), chunk)]
        for j in range(chunk // tile):
            out_keys[:, pl.ds(pl.multiple_of(i * chunk + j * tile, tile), tile)] = k[j * tile : (j + 1) * tile].T
        pages = k.astype(jnp.float32).reshape(chunk // PAGE, PAGE, size)
        to = pl.ds(pl.multiple_of(i * 8, 8), 8)
        high[to] = jnp.max(pages, axis=1)
        low[to] = jnp.min(pages, axis=1)

    out_high[...] = high[...].astype(out_high.dtype)
    out_low[...] = low[...].astype(out_low.dtype)

    own_values.wait()
    all_early = all_of(staged, out_values, for_early, ORDER, EARLY)
    all_early.wait()
    all_keys.wait_send()
    all_across = all_of(values, out_values, for_across, across, PIECES - EARLY)
    all_across.wait()

    @pl.when(core == 1)
    def _():
        all_along = all_of(values, out_values, for_along, along, PIECES - EARLY)
        all_along.wait()


def exchange_late(values, after, late, semaphores):
    del after
    blocks, rows, _ = late.shape
    x, z, core = position()
    far, near = indices(x, z, core)
    along = [offset for offset in ORDER if not offset[2]]

    def partner(offset):
        f, n = indices((x + offset[0]) % 4, (z + offset[1]) % 2, core)
        return f * 4 + n, {"farcp": f, "nearcp": n}

    @pl.when(core == 0)
    def _():
        barrier = pltpu.get_barrier_semaphore()
        for offset in along:
            _, device = partner(offset)
            pl.semaphore_signal(barrier, inc=1, device_id=device, device_id_type=MESH)
        pl.semaphore_wait(barrier, len(along))
        step = rows // (PIECES - EARLY)
        for piece in range(PIECES - EARLY):
            for offset in along:
                to, device = partner(offset)
                pltpu.make_async_remote_copy(
                    values.at[to, pl.ds(values.shape[1] - rows + piece * step, step)],
                    late.at[far * 4 + near, pl.ds(piece * step, step)],
                    semaphores.at[0],
                    semaphores.at[1],
                    device_id=device,
                    device_id_type=MESH,
                ).start()
        every = (pl.ds(0, len(along)), pl.ds(0, rows))
        pltpu.make_async_remote_copy(
            values.at[every],
            late.at[every],
            semaphores.at[0],
            semaphores.at[1],
            device_id={"farcp": far, "nearcp": near},
            device_id_type=MESH,
        ).wait()


def write_late(late, _, values, done):
    rows = late.shape[1]
    x, z, core = position()

    @pl.when(core == 0)
    def _():
        copies = []
        for i, offset in enumerate([offset for offset in ORDER if not offset[2]]):
            f, n = indices((x + offset[0]) % 4, (z + offset[1]) % 2, core)
            b = f * 4 + n
            copies.append(
                pltpu.make_async_copy(
                    late.at[b], values.at[b, pl.ds(values.shape[1] - rows, rows)], done.at[i]
                )
            )
            copies[-1].start()
        for one in copies:
            one.wait()


def write_out(keys, values, high, low, out_keys, out_values, out_high, out_low, done):
    copies = [(high, out_high), (low, out_low)]
    for a, b in ((keys, out_keys), (values, out_values)):
        step = a.shape[0] // 8
        copies += [(a.at[pl.ds(i * step, step)], b.at[pl.ds(i * step, step)]) for i in range(8)]
    copies = [pltpu.make_async_copy(a, b, done.at[i]) for i, (a, b) in enumerate(copies)]
    for one in copies:
        one.start()
    for one in copies:
        one.wait()


def per_device(raw_keys, raw_values, turn_angle):
    blocks, rows, _, size = raw_keys.shape
    length = blocks * rows
    kind = raw_keys.dtype
    keys = raw_keys.reshape(blocks, rows, size)
    values = raw_values.reshape(blocks, rows, size)
    angle = turn_angle.T
    anywhere = pl.BlockSpec(memory_space=pl.ANY)
    inside = pl.BlockSpec(memory_space=pltpu.VMEM)
    moved = pl.pallas_call(
        exchange,
        out_shape=(
            pltpu.VMEM((size, length), kind),
            pltpu.VMEM((blocks, rows, size), kind),
            pltpu.VMEM((length // PAGE, size), kind),
            pltpu.VMEM((length // PAGE, size), kind),
        ),
        in_specs=[anywhere] * 3,
        out_specs=(inside,) * 4,
        scratch_shapes=[
            pltpu.VMEM((blocks, rows // PIECES * EARLY, size), kind),
            pltpu.VMEM((blocks, rows, size), kind),
            pltpu.VMEM((blocks, rows, size), kind),
            pltpu.VMEM((size // 2, rows), jnp.float32),
            pltpu.VMEM((rows, size), jnp.float32),
            pltpu.VMEM((rows, size), jnp.float32),
            pltpu.VMEM((length // PAGE, size), jnp.float32),
            pltpu.VMEM((length // PAGE, size), jnp.float32),
        ]
        + [pltpu.SemaphoreType.DMA((2,))] * 4
        + [pltpu.SemaphoreType.DMA((4,))],
        compiler_params=pltpu.CompilerParams(
            collective_id=0, has_side_effects=True, vmem_limit_bytes=48 << 20
        ),
    )(keys, values, angle)
    k, v, high, low = moved
    moved = [pltpu.with_memory_space_constraint(a, pltpu.VMEM) for a in (k, v, high, low)]
    k, v, high, low = pl.pallas_call(
        write_out,
        out_shape=tuple(pltpu.HBM(a.shape, a.dtype) for a in moved),
        in_specs=[inside] * 4,
        out_specs=(anywhere,) * 4,
        scratch_shapes=[pltpu.SemaphoreType.DMA((18,))],
        compiler_params=pltpu.CompilerParams(vmem_limit_bytes=1 << 20),
    )(*moved)
    last = rows // PIECES * (PIECES - EARLY)
    late = pl.pallas_call(
        exchange_late,
        out_shape=pltpu.VMEM((blocks, last, size), kind),
        in_specs=[anywhere] * 2,
        out_specs=inside,
        scratch_shapes=[pltpu.SemaphoreType.DMA((2,))],
        compiler_params=pltpu.CompilerParams(
            collective_id=1, has_side_effects=True, vmem_limit_bytes=58 << 20
        ),
    )(values, low)
    late = pltpu.with_memory_space_constraint(late, pltpu.VMEM)
    v = pl.pallas_call(
        write_late,
        out_shape=pltpu.HBM(v.shape, kind),
        in_specs=[inside, anywhere],
        out_specs=anywhere,
        input_output_aliases={1: 0},
        scratch_shapes=[pltpu.SemaphoreType.DMA((len(ORDER),))],
        compiler_params=pltpu.CompilerParams(vmem_limit_bytes=1 << 20),
    )(late, v)
    return k[None, None], v.reshape(1, length, 1, size), high[None, :, None], low[None, :, None]


def solution(mesh):
    return jax.shard_map(
        per_device,
        mesh=mesh,
        in_specs=(
            P(None, ("farcp", "nearcp"), "heads", None),
            P(None, ("farcp", "nearcp"), "heads", None),
            P(),
        ),
        out_specs=(
            P(("farcp", "nearcp"), "heads", None, None),
            P(("farcp", "nearcp"), None, "heads", None),
            P(("farcp", "nearcp"), None, "heads", None),
            P(("farcp", "nearcp"), None, "heads", None),
        ),
        check_vma=False,
    )
```
